32 devices in a mesh: grp: 4 (over y, core), dev: 8 (over z, x).
Axes of the slice: x: 2, y: 2, z: 4, core: 2. Of those that a mesh axis runs over, the one named last changes fastest.
Arguments:
- targets: float32 [64, 16384], P(None, ('grp', 'dev')), may hold values from -1.7 to 1.7
- source_grid: int32 [64, 4096], P(None, ('grp', 'dev')), may hold values from -1331000 to 1331000
- source_weight: int32 [1, 4096], P(None, ('grp', 'dev')), may hold values from 1 to 1024
Outputs:
- kernel_sum: float32 [16384], P(('grp', 'dev'))
The draws below stay inside these ranges and needn't reach their ends.
All inputs are finite; a program needn't handle non-finite values.
Results may differ from the reference program's by a relative error of at most 0.00017.
Values sent between devices are 32-bit elements; how exact they have to be, the bound alone decides.
No kernel may reach another device: no remote copies, remote signals or barrier semaphores. Data moves between devices by JAX's collectives and lax.ppermute only.
A program may use at most 64 MiB of HBM per device.

```python
import jax
import jax.numpy as jnp
from jax import lax

D = 64
TGT_DEV = 512
SRC_DEV = 128
TARGETS = 16384
SOURCES = 4096
N_DEV = 8


def centre_table(key):
    centre_count = max(SOURCES // SRC_DEV, 1)
    return jax.random.randint(jax.random.fold_in(key, 11), (D, centre_count), -495000, 495001)


def draw_source_grid(key, part):
    centre_count = max(SOURCES // SRC_DEV, 1)
    centres = centre_table(key)
    owner = jax.random.permutation(jax.random.fold_in(key, 12), SOURCES) % centre_count
    first_noise = jax.random.randint(jax.random.fold_in(key, 13), (D, SOURCES), -418000, 418001)
    second_noise = jax.random.randint(jax.random.fold_in(key, 14), (D, SOURCES), -418000, 418001)
    return (centres[:, owner] + first_noise + second_noise).astype(jnp.int32)


def draw_targets(key, part):
    centre_count = max(SOURCES // SRC_DEV, 1)
    centres = centre_table(key).astype(jnp.float32) / 1048576.0
    owner = jax.random.randint(jax.random.fold_in(key, 15), (TARGETS,), 0, centre_count)
    base = centres[:, owner]
    noise = jnp.clip(0.326 * jax.random.normal(jax.random.fold_in(key, 17), (D, TARGETS), jnp.float32), -1.2, 1.2)
    return (base + noise).astype(jnp.float32)


def place_ends(values, key, smallest, top_value):
    index_at = [jax.random.randint(jax.random.fold_in(key, axis), (), 0, length) for axis, length in enumerate(values.shape)]
    widest = values.shape.index(max(values.shape))
    neighbour = index_at[:widest] + [(index_at[widest] + 1) % values.shape[widest]] + index_at[widest + 1:]
    return values.at[tuple(index_at)].set(smallest).at[tuple(neighbour)].set(top_value)


def setup_inputs(seed: int = 0) -> dict:
    arg_keys = jax.random.split(jax.random.key(seed), 4)
    return {
        "targets": draw_targets(jax.random.fold_in(arg_keys[3], 71), 0),
        "source_grid": draw_source_grid(jax.random.fold_in(arg_keys[3], 71), 0),
        "source_weight": place_ends(jax.random.randint(arg_keys[2], (1, SOURCES), 1, 1025), jax.random.fold_in(arg_keys[2], 1), 1, 1024).astype(jnp.int32),
    }


KERNEL_RATE = 0.7


def block_sum(tgt_rows, src_points, src_mass):
    tgt_norm = jnp.sum(tgt_rows * tgt_rows, axis=0)
    src_norm = jnp.sum(src_points * src_points, axis=0)
    inner_prod = lax.dot_general(tgt_rows, src_points, (((0,), (0,)), ((), ())), precision=lax.Precision.HIGHEST, preferred_element_type=jnp.float32)
    distance = tgt_norm[:, None] + src_norm[None, :] - 2.0 * inner_prod
    kernel = jnp.exp(-KERNEL_RATE * distance)
    return jnp.dot(kernel, src_mass[0], precision=lax.Precision.HIGHEST, preferred_element_type=jnp.float32)


def reference(targets, source_grid, source_weight):
    points = source_grid.astype(jnp.float32) / 1048576.0
    masses = source_weight.astype(jnp.float32) / 16.0
    rows_block = TGT_DEV * min(8, N_DEV)
    cols_block = SRC_DEV * 4
    count_cols = SOURCES // cols_block
    point_blocks = jnp.transpose(points.reshape(D, count_cols, cols_block), (1, 0, 2))
    mass_blocks = jnp.transpose(masses.reshape(1, count_cols, cols_block), (1, 0, 2))
    target_blocks = jnp.transpose(targets.reshape(D, TARGETS // rows_block, rows_block), (1, 0, 2))

    def one_target_block(tgt_rows):
        def advance(running, source_pair):
            return running + block_sum(tgt_rows, source_pair[0], source_pair[1]), None
        result, unused = lax.scan(advance, jnp.zeros((rows_block,), jnp.float32), (point_blocks, mass_blocks))
        return result

    sums = lax.map(one_target_block, target_blocks)
    return sums.reshape(TARGETS)
```

```python
import functools
import math

import jax
import jax.numpy as jnp
from jax import lax
from jax.experimental import pallas as pl
from jax.experimental.pallas import tpu as pltpu
from jax.sharding import PartitionSpec as P

KERNEL_RATE = 0.7
RATE_LOG2 = KERNEL_RATE * math.log2(math.e)
WEIGHT_ROWS = 8


def route(count, step):
    if count & (count - 1) == 0:
        return [(i, i ^ step) for i in range(count)]
    return [(i, (i + step) % count) for i in range(count)]


def back_route(count, step):
    return [(to, at) for at, to in route(count, step)]


def split(values):
    high = values.astype(jnp.bfloat16)
    return high, (values - high.astype(jnp.float32)).astype(jnp.bfloat16)


def sums_kernel(count_tgt, count_src, *refs):
    tgt_refs, src_refs = refs[:count_tgt], refs[count_tgt : count_tgt + count_src]
    out_refs = refs[count_tgt + count_src : 2 * count_tgt + count_src]
    tgt_parts, tgt_term = refs[2 * count_tgt + count_src :]
    dim, width = tgt_refs[0].shape
    for i, ref in enumerate(tgt_refs):
        tgt = ref[...]
        cols = pl.ds(i * width, width)
        norm = jnp.sum(tgt * tgt, axis=0, keepdims=True)
        tgt_term[:, cols] = jnp.broadcast_to(-RATE_LOG2 * norm, (8, width))
        high, low = split(tgt * (2.0 * RATE_LOG2))
        tgt_parts[:, cols] = jnp.concatenate([high, low, high, low], axis=0)
    running = [jnp.zeros((8, width), jnp.float32) for _ in range(count_tgt)]
    for ref in src_refs:
        points = ref[0:dim, :].astype(jnp.float32) * (1.0 / 1048576.0)
        masses = ref[dim : dim + WEIGHT_ROWS, :].astype(jnp.float32) * (1.0 / 16.0)
        src_count = points.shape[1]
        norm = jnp.sum(points * points, axis=0, keepdims=True)
        term = jnp.log2(masses) - RATE_LOG2 * norm
        term = jnp.broadcast_to(term[0:1], (128, src_count)).T
        term = jnp.concatenate([term] * (width // 128), axis=1)
        high, low = split(points)
        src_parts = jnp.concatenate([high, high, low, low], axis=0).T
        for i in range(count_tgt):
            cols = pl.ds(i * width, width)
            inner = jnp.dot(src_parts, tgt_parts[:, cols], preferred_element_type=jnp.float32)
            value = jnp.exp2(inner + tgt_term[0:1, cols] + term)
            running[i] = running[i] + jnp.sum(value.reshape(src_count // 8, 8, width), axis=0)
    for i, ref in enumerate(out_refs):
        ref[...] = jnp.sum(running[i], axis=0, keepdims=True)


def partial_sums(tgts, srcs):
    count_tgt, count_src = len(tgts), len(srcs)
    dim, width = tgts[0].shape
    pairs = count_tgt * width * sum(src.shape[1] for src in srcs)
    in_vmem = pl.BlockSpec(memory_space=pltpu.VMEM)
    return pl.pallas_call(
        functools.partial(sums_kernel, count_tgt, count_src),
        out_shape=[jax.ShapeDtypeStruct((1, width), jnp.float32)] * count_tgt,
        in_specs=[in_vmem] * (count_tgt + count_src),
        out_specs=[in_vmem] * count_tgt,
        scratch_shapes=[
            pltpu.VMEM((4 * dim, count_tgt * width), jnp.bfloat16),
            pltpu.VMEM((8, count_tgt * width), jnp.float32),
        ],
        cost_estimate=pl.CostEstimate(
            flops=8 * dim * pairs, bytes_accessed=4 * dim * count_tgt * width, transcendentals=pairs
        ),
    )(*tgts, *srcs)


def shards(targets, source_grid, source_weight):
    groups, devices = lax.axis_size("grp"), lax.axis_size("dev")
    tgts = [targets] + [lax.ppermute(targets, "grp", route(groups, k)) for k in range(1, groups)]
    weights = jnp.broadcast_to(source_weight, (WEIGHT_ROWS, source_weight.shape[1]))
    block = jnp.concatenate([source_grid, weights], axis=0)
    couples = devices
    if devices % 2 == 0:
        block = jnp.concatenate([block, lax.ppermute(block, "dev", [(i, i ^ 1) for i in range(devices)])], axis=1)
        couples = devices // 2
    each = devices // couples
    srcs = [block]
    for k in range(1, couples):
        pairs = [
            (each * i + j, each * ((i + k) % couples) + j) for i in range(couples) for j in range(each)
        ]
        srcs.append(lax.ppermute(block, "dev", pairs))
    sums = partial_sums(tgts, srcs)
    total = sums[0]
    for k in range(1, groups):
        total = total + lax.ppermute(sums[k], "grp", back_route(groups, k))
    return total.reshape(targets.shape[1])


def solution(mesh):
    in_specs = (P(None, ("grp", "dev")), P(None, ("grp", "dev")), P(None, ("grp", "dev")))
    out_specs = P(("grp", "dev"))
    return jax.shard_map(shards, mesh=mesh, in_specs=in_specs, out_specs=out_specs, check_vma=False)
```

```python
import functools
import math

import jax
import jax.numpy as jnp
from jax import lax
from jax.experimental import pallas as pl
from jax.experimental.pallas import tpu as pltpu
from jax.sharding import PartitionSpec as P


KERNEL_RATE = 0.7
RATE_LOG2 = KERNEL_RATE * math.log2(math.e)
WEIGHT_ROWS = 8
AXES = ("grp", "dev")
VMEM_LIMIT = 16 * 1024 * 1024
DEAL = (0, 1, 1, 0, 1, 0, 1)


def split(values):
    high = values.astype(jnp.bfloat16)
    return high, (values - high.astype(jnp.float32)).astype(jnp.bfloat16)


def sums_kernel(count_tgt, src_counts, count_add, *refs):
    count_src = len(src_counts)
    tgt_refs, src_refs = refs[:count_tgt], refs[count_tgt : count_tgt + count_src]
    refs = refs[count_tgt + count_src :]
    add_refs, out_refs = refs[:count_add], refs[count_add : count_add + count_tgt]
    tgt_parts, tgt_term = refs[count_add + count_tgt :]
    dim, width = tgt_refs[0].shape
    for i, ref in enumerate(tgt_refs):
        tgt = ref[...]
        cols = pl.ds(i * width, width)
        norm = jnp.sum(tgt * tgt, axis=0, keepdims=True)
        tgt_term[:, cols] = jnp.broadcast_to(-RATE_LOG2 * norm, (8, width))
        high, low = split(tgt * (2.0 * RATE_LOG2))
        tgt_parts[:, cols] = jnp.concatenate([high, low, high, low], axis=0)
    running = [jnp.zeros((8, width), jnp.float32) for _ in range(count_tgt)]
    if count_add:
        running = [ref[...] for ref in add_refs]
    for ref, src_count in zip(src_refs, src_counts):
        points = ref[0:dim, 0:src_count].astype(jnp.float32) * (1.0 / 1048576.0)
        masses = ref[dim : dim + 1, 0:src_count].astype(jnp.float32) * (1.0 / 16.0)
        norm = jnp.sum(points * points, axis=0, keepdims=True)
        term = jnp.log2(masses) - RATE_LOG2 * norm
        term = jnp.broadcast_to(term, (128, src_count)).T
        term = jnp.concatenate([term] * (width // 128), axis=1)
        high, low = split(points)
        src_parts = jnp.concatenate([high, high, low, low], axis=0).T
        for i in range(count_tgt):
            cols = pl.ds(i * width, width)
            inner = jnp.dot(src_parts, tgt_parts[:, cols], preferred_element_type=jnp.float32)
            value = jnp.exp2(inner + tgt_term[0:1, cols] + term)
            running[i] = running[i] + jnp.sum(value.reshape(src_count // 8, 8, width), axis=0)
    for i, ref in enumerate(out_refs):
        if ref.shape[0] == 1:
            ref[...] = jnp.sum(running[i], axis=0, keepdims=True)
        else:
            ref[...] = running[i]


def partial_sums(tgts, srcs, src_counts, adds=(), last=True):
    count_tgt, count_src = len(tgts), len(srcs)
    dim, width = tgts[0].shape
    pairs = count_tgt * width * sum(src_counts)
    in_vmem = pl.BlockSpec(memory_space=pltpu.VMEM)
    return pl.pallas_call(
        functools.partial(sums_kernel, count_tgt, src_counts, len(adds)),
        out_shape=[jax.ShapeDtypeStruct((1 if last else 8, width), jnp.float32)] * count_tgt,
        in_specs=[in_vmem] * (count_tgt + count_src + len(adds)),
        out_specs=[in_vmem] * count_tgt,
        scratch_shapes=[
            pltpu.VMEM((4 * dim, count_tgt * width), jnp.bfloat16),
            pltpu.VMEM((8, count_tgt * width), jnp.float32),
        ],
        compiler_params=pltpu.CompilerParams(vmem_limit_bytes=VMEM_LIMIT),
        cost_estimate=pl.CostEstimate(
            flops=8 * dim * pairs, bytes_accessed=4 * dim * count_tgt * width, transcendentals=pairs
        ),
    )(*tgts, *srcs, *adds)


def moves(groups, devices):
    cores, sides = 2 - groups % 2, 2 - devices % 2
    places = devices // sides
    paired = places & (places - 1) == 0

    def over(change, cores_in=None):
        pairs = []
        for at in range(groups * devices):
            g, d = at // devices, at % devices
            pair, core, place, side = change(g // cores, g % cores, d // sides, d % sides)
            pair, core, place, side = pair % (groups // cores), core % cores, place % places, side % sides
            if cores_in is None or g % cores in cores_in:
                pairs.append((at, (pair * cores + core) * devices + place * sides + side))
        return pairs

    steps = [(p, s) for p in range(places) for s in range(sides) if p or s]
    steps.sort(key=lambda step: (step[0] + step[1], step[0]), reverse=True)
    shares = [[] for _ in range(cores)]
    for i, step in enumerate(steps):
        shares[DEAL[i % len(DEAL)] % cores].append(step)
    shares[0][:2] = shares[0][:2][::-1]
    srcs = []
    for k in range(max(map(len, shares))):
        pairs = []
        for core, share in enumerate(shares):
            if k < len(share):
                far, flip = share[k]
                pairs += over(
                    lambda y, c, p, s, far=far, flip=flip: (y, c, p ^ far if paired else p + far, s + flip), (core,)
                )
        srcs.append(pairs)
    mate = over(lambda y, c, p, s: (y, c + 1, p, s)) if cores == 2 else None
    pairs = [over(lambda y, c, p, s, k=k: (y + k, c, p, s)) for k in range(1, groups // cores)]
    both = [over(lambda y, c, p, s, k=k: (y + k, c + 1, p, s)) for k in range(1, groups // cores)]
    return mate, pairs, both if cores == 2 else [], srcs


def back(move):
    return [(to, at) for at, to in move]


def sent(values, move):
    return lax.ppermute(values, AXES, move)


def placed(part, row, col, size):
    rows, cols = size[0] - row - part.shape[0], size[1] - col - part.shape[1]
    return lax.pad(part, jnp.zeros((), part.dtype), [(row, rows, 0), (col, cols, 0)])


def body(targets, source_grid, source_weight):
    groups, devices = lax.axis_size("grp"), lax.axis_size("dev")
    mate, pairs, both, src_moves = moves(groups, devices)
    dim, count = source_grid.shape
    others = [sent(targets, move) for move in pairs]

    size = (dim + WEIGHT_ROWS, count * (1 if mate is None else 2))
    block = placed(source_grid, 0, 0, size) + placed(source_weight, dim, 0, size)
    if mate is not None:
        block = lax.optimization_barrier(block)
        block = block + placed(sent(source_grid, mate), 0, count, size)
        block = block + placed(sent(source_weight, mate), dim, count, size)
    srcs = [block] + [sent(block, move) for move in src_moves]
    counts = [count] + [src.shape[1] for src in srcs[1:]]

    own = [targets]
    if mate is not None:
        others += [sent(other, mate) for other in others]
        own += [sent(targets, mate)]
    sums = ()
    cuts = sorted({0, min(2, len(srcs) - 1), len(srcs) - 1, len(srcs)})
    for low, high in zip(cuts, cuts[1:]):
        sums = partial_sums(others, srcs[low:high], counts[low:high], sums, high == len(srcs))
    mine = partial_sums(own, srcs, counts)
    total = mine[0]
    for part in mine[1:]:
        total = total + sent(part, mate)
    for part, move in zip(sums, pairs + both):
        total = total + sent(part, back(move))
    return total.reshape(targets.shape[1])


def solution(mesh):
    in_specs = (P(None, ("grp", "dev")), P(None, ("grp", "dev")), P(None, ("grp", "dev")))
    out_specs = P(("grp", "dev"))
    return jax.shard_map(body, mesh=mesh, in_specs=in_specs, out_specs=out_specs, check_vma=False)
```

```python
import functools
import math

import jax
import jax.numpy as jnp
from jax import lax
from jax.experimental import pallas as pl
from jax.experimental.pallas import tpu as pltpu
from jax.sharding import PartitionSpec as P


KERNEL_RATE = 0.7
RATE_LOG2 = KERNEL_RATE * math.log2(math.e)
WEIGHT_ROWS = 8
AXES = ("grp", "dev")
VMEM_LIMIT = 16 * 1024 * 1024
DEAL = (0, 1, 1, 0, 1, 0, 1)


def split(values):
    high = values.astype(jnp.bfloat16)
    return high, (values - high.astype(jnp.float32)).astype(jnp.bfloat16)


def sums_kernel(count_tgt, src_counts, count_add, *refs):
    count_src = len(src_counts)
    tgt_refs, src_refs = refs[:count_tgt], refs[count_tgt : count_tgt + count_src]
    refs = refs[count_tgt + count_src :]
    add_refs, out_refs = refs[:count_add], refs[count_add : count_add + count_tgt]
    tgt_parts, tgt_term = refs[count_add + count_tgt :]
    dim, width = tgt_refs[0].shape
    for i, ref in enumerate(tgt_refs):
        tgt = ref[...]
        cols = pl.ds(i * width, width)
        norm = jnp.sum(tgt * tgt, axis=0, keepdims=True)
        tgt_term[:, cols] = jnp.broadcast_to(-RATE_LOG2 * norm, (8, width))
        high, low = split(tgt * (2.0 * RATE_LOG2))
        tgt_parts[:, cols] = jnp.concatenate([high, low, high, low], axis=0)
    running = [jnp.zeros((8, width), jnp.float32) for _ in range(count_tgt)]
    if count_add:
        running = [ref[...] for ref in add_refs]
    for ref, src_count in zip(src_refs, src_counts):
        points = ref[0:dim, 0:src_count].astype(jnp.float32) * (1.0 / 1048576.0)
        masses = ref[dim : dim + 1, 0:src_count].astype(jnp.float32) * (1.0 / 16.0)
        norm = jnp.sum(points * points, axis=0, keepdims=True)
        term = jnp.log2(masses) - RATE_LOG2 * norm
        term = jnp.broadcast_to(term, (128, src_count)).T
        term = jnp.concatenate([term] * (width // 128), axis=1)
        high, low = split(points)
        src_parts = jnp.concatenate([high, high, low, low], axis=0).T
        for i in range(count_tgt):
            cols = pl.ds(i * width, width)
            inner = jnp.dot(src_parts, tgt_parts[:, cols], preferred_element_type=jnp.float32)
            value = jnp.exp2(inner + tgt_term[0:1, cols] + term)
            running[i] = running[i] + jnp.sum(value.reshape(src_count // 8, 8, width), axis=0)
    for i, ref in enumerate(out_refs):
        if ref.shape[0] == 1:
            ref[...] = jnp.sum(running[i], axis=0, keepdims=True)
        else:
            ref[...] = running[i]


def partial_sums(tgts, srcs, src_counts, adds=(), last=True):
    count_tgt, count_src = len(tgts), len(srcs)
    dim, width = tgts[0].shape
    pairs = count_tgt * width * sum(src_counts)
    in_vmem = pl.BlockSpec(memory_space=pltpu.VMEM)
    return pl.pallas_call(
        functools.partial(sums_kernel, count_tgt, src_counts, len(adds)),
        out_shape=[jax.ShapeDtypeStruct((1 if last else 8, width), jnp.float32)] * count_tgt,
        in_specs=[in_vmem] * (count_tgt + count_src + len(adds)),
        out_specs=[in_vmem] * count_tgt,
        scratch_shapes=[
            pltpu.VMEM((4 * dim, count_tgt * width), jnp.bfloat16),
            pltpu.VMEM((8, count_tgt * width), jnp.float32),
        ],
        compiler_params=pltpu.CompilerParams(vmem_limit_bytes=VMEM_LIMIT),
        cost_estimate=pl.CostEstimate(
            flops=8 * dim * pairs, bytes_accessed=4 * dim * count_tgt * width, transcendentals=pairs
        ),
    )(*tgts, *srcs, *adds)


def moves(groups, devices):
    cores, sides = 2 - groups % 2, 2 - devices % 2
    places = devices // sides
    paired = places & (places - 1) == 0

    def over(change, cores_in=None):
        pairs = []
        for at in range(groups * devices):
            g, d = at // devices, at % devices
            pair, core, place, side = change(g // cores, g % cores, d // sides, d % sides)
            pair, core, place, side = pair % (groups // cores), core % cores, place % places, side % sides
            if cores_in is None or g % cores in cores_in:
                pairs.append((at, (pair * cores + core) * devices + place * sides + side))
        return pairs

    steps = [(p, s) for p in range(places) for s in range(sides) if p or s]
    steps.sort(key=lambda step: (step[0] + step[1], step[0]), reverse=True)
    shares = [[] for _ in range(cores)]
    half = [steps.pop()] if cores == 2 and steps else []
    for i, step in enumerate(steps):
        shares[DEAL[i % len(DEAL)] % cores].append(step)
    shares[0][:2] = shares[0][:2][::-1]
    srcs = []
    for k in range(max(map(len, shares))):
        pairs = []
        for core, share in enumerate(shares):
            if k < len(share):
                far, flip = share[k]
                pairs += over(
                    lambda y, c, p, s, far=far, flip=flip: (y, c, p ^ far if paired else p + far, s + flip), (core,)
                )
        srcs.append(pairs)
    for far, flip in half:
        srcs.append(over(lambda y, c, p, s: (y, c, p ^ far if paired else p + far, s + flip)))
    mate = over(lambda y, c, p, s: (y, c + 1, p, s)) if cores == 2 else None
    pairs = [over(lambda y, c, p, s, k=k: (y + k, c, p, s)) for k in range(1, groups // cores)]
    both = [over(lambda y, c, p, s, k=k: (y + k, c + 1, p, s)) for k in range(1, groups // cores)]
    return mate, pairs, both if cores == 2 else [], srcs


def back(move):
    return [(to, at) for at, to in move]


def sent(values, move):
    return lax.ppermute(values, AXES, move)


def placed(part, row, col, size):
    rows, cols = size[0] - row - part.shape[0], size[1] - col - part.shape[1]
    return lax.pad(part, jnp.zeros((), part.dtype), [(row, rows, 0), (col, cols, 0)])


def body(targets, source_grid, source_weight):
    groups, devices = lax.axis_size("grp"), lax.axis_size("dev")
    mate, pairs, both, src_moves = moves(groups, devices)
    dim, count = source_grid.shape
    others = [sent(targets, move) for move in pairs]

    size = (dim + WEIGHT_ROWS, count * (1 if mate is None else 2))
    block = placed(source_grid, 0, 0, size) + placed(source_weight, dim, 0, size)
    if mate is not None:
        block = lax.optimization_barrier(block)
        block = block + placed(sent(source_grid, mate), 0, count, size)
        block = block + placed(sent(source_weight, mate), dim, count, size)
    single = block if mate is None else block[:, :count]
    srcs = [block]
    for i, move in enumerate(src_moves):
        srcs.append(sent(single if i == len(src_moves) - 1 else block, move))
    counts = [count] + [src.shape[1] for src in srcs[1:]]

    own = [targets]
    if mate is not None:
        others += [sent(other, mate) for other in others]
        own += [sent(targets, mate)]
    sums = ()
    index = list(range(len(srcs)))
    late = sorted({index[-1], min(2, index[-1])})
    early = [i for i in index[:2] if i not in late]
    groups_of = [part for part in (early, [i for i in index if i not in early + late], late) if part]
    for i, part in enumerate(groups_of):
        is_last = i == len(groups_of) - 1
        sums = partial_sums(others, [srcs[k] for k in part], [counts[k] for k in part], sums, is_last)
    mine = partial_sums(own, srcs, counts)
    total = mine[0]
    for part in mine[1:]:
        total = total + sent(part, mate)
    for part, move in zip(sums, pairs + both):
        total = total + sent(part, back(move))
    return total.reshape(targets.shape[1])


def solution(mesh):
    in_specs = (P(None, ("grp", "dev")), P(None, ("grp", "dev")), P(None, ("grp", "dev")))
    out_specs = P(("grp", "dev"))
    return jax.shard_map(body, mesh=mesh, in_specs=in_specs, out_specs=out_specs, check_vma=False)
```
